32 devices in a mesh: gx: 8 (over y, x, core), gy: 4 (over z).
Axes of the slice: x: 2, y: 2, z: 4, core: 2. Of those that a mesh axis runs over, the one named last changes fastest.
Arguments:
- object_field: float32 [2, 256, 512], P(None, 'gy', 'gx'), may hold values from -1 to 1
- probe_modes: float32 [2, 1024, 128], P(None, ('gy', 'gx')), may hold values from -1.5 to 1.5
- positions: int32 [4, 8, 12, 2], P('gy', 'gx'), may hold values from 4 to 60, as said below
- amplitudes: float32 [4, 8, 12, 128, 128], P('gy', 'gx'), may hold values from 0 to 2
Outputs:
- object_out: float32 [2, 256, 512], P(None, 'gy', 'gx')
- probe_out: float32 [2, 1024, 128], P(None, ('gy', 'gx'))
The draws below stay inside these ranges and needn't reach their ends.
Inputs may be any that keep to these rules, and one draw needn't show every extreme that they name: `positions`: each entry is a (row, column) inside its own tile; the centres of one tile lie at distinct cells of the 16 grid, each moved from the cell's middle by at most 4 cells along each dimension.
All inputs are finite; a program needn't handle non-finite values.
Results may differ from the reference program's by a relative error of at most 0.00065.
The reference program's roundings to bfloat16 on the way count: a program that leaves them out, or rounds other values in their place, can miss the bound.
Values sent between devices are 32-bit elements; how exact they have to be, the bound alone decides.
A program may use at most 64 MiB of HBM per device.

```python
import math
import jax
import jax.numpy as jnp
from jax import lax

PROBE = 128
MODES = 8
TILE = 64
STRIDE = 16
POS_DEV = 12
ITERS = 2
TILES_Y = 4
TILES_X = 8
NY = 256
NX = 512


def draw_positions(key, part):
    grid_cells = TILE // STRIDE
    tile_count = TILES_Y * TILES_X
    keys = jax.random.split(jax.random.fold_in(key, 11), tile_count)

    def one_tile(subkey):
        chosen = jax.random.permutation(subkey, grid_cells * grid_cells)[:POS_DEV]
        jitter = jax.random.randint(jax.random.fold_in(subkey, 3), (POS_DEV, 2), -4, 5)
        cells = jnp.stack([chosen // grid_cells, chosen % grid_cells], axis=1)
        return cells * STRIDE + STRIDE // 2 + jitter
    return jax.vmap(one_tile)(keys).reshape(TILES_Y, TILES_X, POS_DEV, 2).astype(jnp.int32)


def draw_object_field(key, part):
    base = jax.random.fold_in(key, 23)
    magnitude_key = jax.random.fold_in(base, 1)
    phase_key = jax.random.fold_in(base, 2)
    magnitude = jax.random.uniform(magnitude_key, (NY, NX), jnp.float32, 0.5, 1.0)
    phase = jax.random.uniform(phase_key, (NY, NX), jnp.float32, -0.6, 0.6)
    return jnp.stack([magnitude * jnp.cos(phase), magnitude * jnp.sin(phase)]).astype(jnp.float32)


def steps_of(stream_key, dims, shards, least, high):
    level = 1.0
    for position, blocks in shards:
        heights = jax.random.uniform(jax.random.fold_in(jax.random.fold_in(stream_key, 6), position), (blocks,), jnp.float32, least / len(shards), high / len(shards))
        level = level * jnp.repeat(jnp.exp(heights), dims[position] // blocks).reshape((-1,) + (1,) * (len(dims) - 1 - position))
    return level


def normal_values(rng, dims, deviation, bound, shards=(), kind=jnp.bfloat16):
    values = jax.random.normal(rng, dims, jnp.float32) * deviation
    if len(shards) > 0:
        values = steps_of(rng, dims, shards, -0.22, 0.18) * values
    return jnp.clip(values, min=-bound, max=bound).astype(kind)


def setup_inputs(seed: int = 0) -> dict:
    streams_of = jax.random.split(jax.random.key(seed), 5)
    return {
        "object_field": draw_object_field(jax.random.fold_in(streams_of[4], 71), 0),
        "probe_modes": normal_values(streams_of[1], (2, MODES * PROBE, PROBE), 0.25, 1.5, ((1, 32),), jnp.float32),
        "positions": draw_positions(jax.random.fold_in(streams_of[4], 71), 0),
        "amplitudes": jnp.clip(2.0 * jax.random.uniform(streams_of[3], (TILES_Y, TILES_X, POS_DEV, PROBE, PROBE), jnp.float32) ** steps_of(streams_of[3], (TILES_Y, TILES_X, POS_DEV, PROBE, PROBE), ((0, 4), (1, 8)), -0.2, 0.2), 0.0, 2.0),
    }


SOFT_FLOOR = 0.05
OBJECT_REG = 1.0
PROBE_REG = 1.0

def tables(probe_side, sign_flip):
    indices = jnp.arange(probe_side, dtype=jnp.int32)
    phases = indices[:, None] * indices[None, :] % probe_side
    angles = phases.astype(jnp.float32) * (2.0 * math.pi / probe_side)
    factor = 1.0 / math.sqrt(probe_side)
    cosine = jnp.cos(angles) * factor
    sine_part = sign_flip * jnp.sin(angles) * factor
    left_op = jnp.stack([jnp.stack([cosine, -sine_part]), jnp.stack([sine_part, cosine])]).transpose(0, 2, 1, 3)
    right_op = jnp.stack([jnp.stack([cosine, sine_part]), jnp.stack([-sine_part, cosine])]).transpose(0, 2, 1, 3)
    return (left_op.astype(jnp.bfloat16), right_op.astype(jnp.bfloat16))

def transform(signal, operators):
    left_op, right_op = operators
    signal = lax.optimization_barrier(signal)
    halfway = jnp.einsum('dpcr,crmq->dpmq', left_op.astype(jnp.float32), signal.astype(jnp.float32), precision=lax.Precision.HIGHEST).astype(jnp.bfloat16)
    halfway = lax.optimization_barrier(halfway)
    return jnp.einsum('crmq,cqdk->drmk', halfway.astype(jnp.float32), right_op.astype(jnp.float32), precision=lax.Precision.HIGHEST)

def position_terms(patch_obj, probe, measured, forward, inverse):
    obj_real = patch_obj[0][:, None, :]
    obj_imag = patch_obj[1][:, None, :]
    wave_real = probe[0] * obj_real - probe[1] * obj_imag
    wave_imag = probe[0] * obj_imag + probe[1] * obj_real
    signal = jnp.stack([wave_real, wave_imag]).astype(jnp.bfloat16)
    spectrum = transform(signal, forward)
    intensity = lax.optimization_barrier(jnp.sum(spectrum[0] * spectrum[0] + spectrum[1] * spectrum[1], axis=1))
    shrink = 1.0 - measured / jnp.sqrt(intensity + SOFT_FLOOR)
    residual = (spectrum * shrink[None, :, None, :]).astype(jnp.bfloat16)
    change = transform(residual, inverse)
    grad_real = lax.optimization_barrier(jnp.sum(probe[0] * change[0] + probe[1] * change[1], axis=1))
    grad_imag = lax.optimization_barrier(jnp.sum(probe[0] * change[1] - probe[1] * change[0], axis=1))
    probe_real = obj_real * change[0] + obj_imag * change[1]
    probe_imag = obj_real * change[1] - obj_imag * change[0]
    weight_probe = patch_obj[0] * patch_obj[0] + patch_obj[1] * patch_obj[1]
    return (jnp.stack([grad_real, grad_imag]), jnp.stack([probe_real, probe_imag]), weight_probe)

def reference(object_field, probe_modes, positions, amplitudes):
    margin = PROBE // 2
    forward = tables(PROBE, -1.0)
    inverse = tables(PROBE, 1.0)
    tile_rows = jnp.arange(TILES_Y, dtype=jnp.int32)[:, None, None] * TILE
    tile_cols = jnp.arange(TILES_X, dtype=jnp.int32)[None, :, None] * TILE
    row_list = (positions[..., 0] + tile_rows).reshape(-1).astype(jnp.int32)
    col_list = (positions[..., 1] + tile_cols).reshape(-1).astype(jnp.int32)
    measured_all = amplitudes.reshape(-1, PROBE, PROBE)
    probe = probe_modes.reshape(2, MODES, PROBE, PROBE).transpose(0, 2, 1, 3)
    current = object_field
    for iteration in range(ITERS):
        padded = jnp.pad(current, ((0, 0), (margin, margin), (margin, margin)))
        weight_obj = lax.optimization_barrier(jnp.sum(probe[0] * probe[0] + probe[1] * probe[1], axis=1))

        def visit(running, visit_item):
            grad_obj, grad_probe, weight_probe = running
            row_at, col_at, measured = visit_item
            zero_index = jnp.int32(0)
            patch_obj = lax.dynamic_slice(padded, (zero_index, row_at, col_at), (2, PROBE, PROBE))
            g_obj, g_probe, w_probe = position_terms(patch_obj, probe, measured, forward, inverse)
            stacked = jnp.concatenate([g_obj, weight_obj[None]], axis=0)
            before = lax.dynamic_slice(grad_obj, (zero_index, row_at, col_at), (3, PROBE, PROBE))
            grad_obj = lax.dynamic_update_slice(grad_obj, before + stacked, (zero_index, row_at, col_at))
            return ((grad_obj, grad_probe + g_probe, weight_probe + w_probe), None)
        initial = (jnp.zeros((3, NY + PROBE, NX + PROBE), jnp.float32), jnp.zeros((2, PROBE, MODES, PROBE), jnp.float32), jnp.zeros((PROBE, PROBE), jnp.float32))
        (grad_obj, grad_probe, weight_probe), _ = lax.scan(visit, initial, (row_list, col_list, measured_all))
        inner = grad_obj[:, margin:margin + NY, margin:margin + NX]
        new_object = current - inner[0:2] / (inner[2] + OBJECT_REG)
        probe = probe - grad_probe / (weight_probe[:, None, :] + PROBE_REG)
        current = new_object
    return (current, probe.transpose(0, 2, 1, 3).reshape(2, MODES * PROBE, PROBE))
```

```python
import math

import jax
import jax.numpy as jnp
from jax import lax
from jax.experimental import pallas as pl
from jax.experimental.pallas import tpu as pltpu
from jax.sharding import PartitionSpec as P

MODES = 8
ITERS = 2
SUBLANES = 8


SOFT_FLOOR = 0.05
OBJECT_REG = 1.0
PROBE_REG = 1.0


def from_behind(block, axis, distance):
    devices = range(lax.axis_size(axis))
    route = [(i - distance, i) for i in devices if i - distance in devices]
    return lax.ppermute(block, axis, route)


def extended_2(array, sides, width):
    for axis, dim in sides:
        peers, length = (lax.axis_size(axis), array.shape[dim])
        up = [(i, (i + 1) % peers) for i in range(peers - 1)]
        down = [(j, i) for i, j in up]
        last = lax.slice_in_dim(array, length - width, length, axis=dim)
        initial = lax.slice_in_dim(array, 0, width, axis=dim)
        before = lax.ppermute(last, axis, up)
        after = lax.ppermute(initial, axis, down)
        array = jnp.concatenate([before, array, after], axis=dim)
    return array


def tables(probe_side, sign_flip):
    indices = jnp.arange(probe_side, dtype=jnp.int32)
    phases = indices[:, None] * indices[None, :] % probe_side
    angles = phases.astype(jnp.float32) * (2.0 * math.pi / probe_side)
    factor = 1.0 / math.sqrt(probe_side)
    cosine = jnp.cos(angles) * factor
    sine_part = sign_flip * jnp.sin(angles) * factor
    left_op = jnp.stack(
        [jnp.stack([cosine, -sine_part]), jnp.stack([sine_part, cosine])]
    ).transpose(0, 2, 1, 3)
    right_op = jnp.stack(
        [jnp.stack([cosine, sine_part]), jnp.stack([-sine_part, cosine])]
    ).transpose(0, 2, 1, 3)
    return (left_op.astype(jnp.bfloat16), right_op.astype(jnp.bfloat16))


def visit_kernel(places, ext_ref, probe_ref, measured_ref, fwd_left, fwd_right, inv_left, inv_right,
                 grad_obj_ref, grad_probe_ref, weight_probe_ref, far_ref, weight_obj_ref):
    count, side, _ = measured_ref.shape
    modes = probe_ref.shape[1] // side
    lanes = ext_ref.shape[2]
    grad_obj_ref[...] = jnp.zeros_like(grad_obj_ref)
    grad_probe_ref[...] = jnp.zeros_like(grad_probe_ref)
    weight_probe_ref[...] = jnp.zeros_like(weight_probe_ref)
    weight = jnp.zeros((side, side), jnp.float32)
    for m in range(modes):
        p_real = probe_ref[0, m * side : (m + 1) * side, :]
        p_imag = probe_ref[1, m * side : (m + 1) * side, :]
        weight += p_real * p_real + p_imag * p_imag
    weight_obj_ref[...] = weight

    def dot(left, right):
        return jnp.dot(left, right, preferred_element_type=jnp.float32)

    def two_sided(left_op, right_op, pair):
        half = dot(left_op[...], pair).astype(jnp.bfloat16)
        results = []
        for k in range(2):
            block = half[:, k * side : (k + 1) * side]
            rows = jnp.concatenate([block[:side], block[side:]], axis=1)
            results.append(dot(rows, right_op[...]))
        return results

    def visit(j, carry):
        row_at = places[j, 0]
        col_at = places[j, 1]
        tall = side + SUBLANES
        shift = lax.rem(row_at, SUBLANES)
        window = pl.ds(pl.multiple_of(row_at - shift, SUBLANES), tall)
        right = lax.rem(lanes - col_at, lanes)
        up = lax.rem(tall - shift, tall)

        def patch_of(i):
            columns = pltpu.roll(ext_ref[i, window, :], right, 1)[:, :side]
            return pltpu.roll(columns, up, 0)[:side]

        o_real = patch_of(0)
        o_imag = patch_of(1)
        weight_probe_ref[...] += o_real * o_real + o_imag * o_imag
        intensity = jnp.zeros((side, side), jnp.float32)
        for m in range(0, modes, 2):
            columns = []
            for k in (m, m + 1):
                p_real = probe_ref[0, k * side : (k + 1) * side, :]
                p_imag = probe_ref[1, k * side : (k + 1) * side, :]
                w_real = (p_real * o_real - p_imag * o_imag).astype(jnp.bfloat16)
                w_imag = (p_real * o_imag + p_imag * o_real).astype(jnp.bfloat16)
                columns.append(jnp.concatenate([w_real, w_imag], axis=0))
            for k, far in enumerate(two_sided(fwd_left, fwd_right, jnp.concatenate(columns, axis=1))):
                far_ref[(m + k) * side : (m + k + 1) * side, :] = far
                intensity += far[:, :side] * far[:, :side] + far[:, side:] * far[:, side:]
        shrink = 1.0 - measured_ref[j] / jnp.sqrt(intensity + SOFT_FLOOR)
        g_real = jnp.zeros((side, side), jnp.float32)
        g_imag = jnp.zeros((side, side), jnp.float32)
        for m in range(0, modes, 2):
            columns = []
            for k in (m, m + 1):
                rows = slice(k * side, (k + 1) * side)
                r_real = (far_ref[rows, :side] * shrink).astype(jnp.bfloat16)
                r_imag = (far_ref[rows, side:] * shrink).astype(jnp.bfloat16)
                columns.append(jnp.concatenate([r_real, r_imag], axis=0))
            for k, change in enumerate(two_sided(inv_left, inv_right, jnp.concatenate(columns, axis=1))):
                rows = slice((m + k) * side, (m + k + 1) * side)
                p_real = probe_ref[0, rows, :]
                p_imag = probe_ref[1, rows, :]
                c_real = change[:, :side]
                c_imag = change[:, side:]
                g_real += p_real * c_real + p_imag * c_imag
                g_imag += p_real * c_imag - p_imag * c_real
                grad_probe_ref[0, rows, :] += o_real * c_real + o_imag * c_imag
                grad_probe_ref[1, rows, :] += o_real * c_imag - o_imag * c_real
        short = jnp.zeros((SUBLANES, side), jnp.float32)
        blank = jnp.zeros((tall, lanes - side), jnp.float32)
        for i, part in enumerate((g_real, g_imag, weight_obj_ref[...])):
            part = jnp.concatenate([part, short], axis=0)
            wide = jnp.concatenate([pltpu.roll(part, shift, 0), blank], axis=1)
            grad_obj_ref[i, window, :] += pltpu.roll(wide, col_at, 1)
        return carry

    lax.fori_loop(0, count, visit, 0)


def flat(operators):
    left_op, right_op = operators
    side = left_op.shape[1]
    return (left_op.reshape(2 * side, 2 * side), right_op.reshape(2 * side, 2 * side))


def gradients(extended, probe, places, measured, forward, inverse):
    side = measured.shape[-1]
    vmem = pl.BlockSpec(memory_space=pltpu.VMEM)
    rows, lanes = extended.shape[1:]
    flops = measured.shape[0] * 4 * 2 * (2 * side) ** 2 * probe.shape[1]
    return pl.pallas_call(
        visit_kernel,
        out_shape=(
            jax.ShapeDtypeStruct((3, rows, lanes), jnp.float32),
            jax.ShapeDtypeStruct(probe.shape, jnp.float32),
            jax.ShapeDtypeStruct((side, side), jnp.float32),
        ),
        in_specs=[pl.BlockSpec(memory_space=pltpu.SMEM)] + [vmem] * 7,
        out_specs=(vmem, vmem, vmem),
        scratch_shapes=[
            pltpu.VMEM((probe.shape[1], 2 * side), jnp.float32),
            pltpu.VMEM((side, side), jnp.float32),
        ],
        compiler_params=pltpu.CompilerParams(vmem_limit_bytes=32 * 1024 * 1024),
        cost_estimate=pl.CostEstimate(flops=flops, bytes_accessed=4 * 1024 * 1024, transcendentals=0),
        name="visits",
    )(places, extended, probe, measured, *forward, *inverse)


def fold_rows(gradient, margin, tile_side):
    extent = gradient.shape[1]
    for direction in (1, -1):
        rim_part = gradient[:, extent - margin :, :] if direction == 1 else gradient[:, :margin, :]
        offset = margin if direction == 1 else tile_side
        arrived = from_behind(rim_part, "gy", direction)
        gradient = gradient.at[:, offset : offset + margin, :].add(arrived)
    return gradient[:, margin : margin + tile_side, :]


def fold_cols(gradient, margin, tile_side):
    extent = gradient.shape[2]
    for direction in (1, -1):
        rim_part = gradient[:, :, extent - margin :] if direction == 1 else gradient[:, :, :margin]
        offset = margin if direction == 1 else tile_side
        arrived = from_behind(rim_part, "gx", direction)
        gradient = gradient.at[:, :, offset : offset + margin].add(arrived)
    return gradient[:, :, margin : margin + tile_side]


def whole_of(own):
    planes = []
    for plane in own:
        planes.append(lax.all_gather(plane, ("gy", "gx"), axis=0, tiled=True))
        own = lax.optimization_barrier(own)
    return jnp.stack(planes)


def scattered_sum(terms):
    planes, rows, side = terms.shape
    down, across = lax.axis_size("gy"), lax.axis_size("gx")
    terms = terms.reshape(planes, down, across, rows // (down * across), side)
    terms = terms.transpose(2, 0, 1, 3, 4)
    terms = lax.all_to_all(terms, "gx", 0, 0, tiled=True).sum(axis=0)
    terms = terms.transpose(1, 0, 2, 3)
    return lax.all_to_all(terms, "gy", 0, 0, tiled=True).sum(axis=0)


def local(object_field, probe_modes, positions, amplitudes):
    probe_side = amplitudes.shape[-1]
    margin = probe_side // 2
    tile_side = object_field.shape[1]
    lanes = -(-(tile_side + probe_side) // 128) * 128
    places = positions.reshape(-1, 2)
    measured = amplitudes.reshape(-1, probe_side, probe_side)
    forward = flat(tables(probe_side, -1.0))
    inverse = flat(tables(probe_side, 1.0))
    own = probe_modes
    probe = whole_of(own)
    current = object_field
    for iteration in range(ITERS):
        extended = extended_2(current, (("gy", 1), ("gx", 2)), margin)
        extended = jnp.pad(extended, ((0, 0), (0, 0), (0, lanes - extended.shape[2])))
        grad_obj, grad_probe, weight_probe = gradients(
            extended, probe, places, measured, forward, inverse
        )
        grad_obj = grad_obj[:, :, : tile_side + probe_side]
        folded = fold_cols(fold_rows(grad_obj, margin, tile_side), margin, tile_side)
        current = current - folded[0:2] / (folded[2] + OBJECT_REG)
        weights = jnp.tile(weight_probe, (MODES, 1))[None]
        totals = scattered_sum(jnp.concatenate([grad_probe, weights]))
        own = own - totals[0:2] / (totals[2:3] + PROBE_REG)
        if iteration < ITERS - 1:
            probe = whole_of(own)
    return (current, own)


def solution(mesh):
    return jax.shard_map(
        local,
        mesh=mesh,
        in_specs=(
            P(None, "gy", "gx"),
            P(None, ("gy", "gx"), None),
            P("gy", "gx", None, None),
            P("gy", "gx", None, None, None),
        ),
        out_specs=(P(None, "gy", "gx"), P(None, ("gy", "gx"), None)),
        check_vma=False,
    )
```

```python
import math

import jax
import jax.numpy as jnp
from jax import lax
from jax.experimental import pallas as pl
from jax.experimental.pallas import tpu as pltpu
from jax.sharding import PartitionSpec as P

MODES = 8
ITERS = 2
SUBLANES = 8


SOFT_FLOOR = 0.05
OBJECT_REG = 1.0
PROBE_REG = 1.0


def from_behind(block, axis, distance):
    devices = range(lax.axis_size(axis))
    route = [(i - distance, i) for i in devices if i - distance in devices]
    return lax.ppermute(block, axis, route)


def extended_2(array, sides, width):
    for axis, dim in sides:
        peers, length = (lax.axis_size(axis), array.shape[dim])
        up = [(i, (i + 1) % peers) for i in range(peers - 1)]
        down = [(j, i) for i, j in up]
        last = lax.slice_in_dim(array, length - width, length, axis=dim)
        initial = lax.slice_in_dim(array, 0, width, axis=dim)
        before = lax.ppermute(last, axis, up)
        after = lax.ppermute(initial, axis, down)
        array = jnp.concatenate([before, array, after], axis=dim)
    return array


def tables(probe_side, sign_flip):
    indices = jnp.arange(probe_side, dtype=jnp.int32)
    phases = indices[:, None] * indices[None, :] % probe_side
    angles = phases.astype(jnp.float32) * (2.0 * math.pi / probe_side)
    factor = 1.0 / math.sqrt(probe_side)
    cosine = jnp.cos(angles) * factor
    sine_part = sign_flip * jnp.sin(angles) * factor
    left_op = jnp.stack(
        [jnp.stack([cosine, -sine_part]), jnp.stack([sine_part, cosine])]
    ).transpose(0, 2, 1, 3)
    right_op = jnp.stack(
        [jnp.stack([cosine, sine_part]), jnp.stack([-sine_part, cosine])]
    ).transpose(0, 2, 1, 3)
    return (left_op.astype(jnp.bfloat16), right_op.astype(jnp.bfloat16))


def visit_kernel(places, ext_ref, probe_ref, measured_ref, fwd_left, fwd_right, inv_left, inv_right,
                 grad_obj_ref, grad_probe_ref, weight_probe_ref, far_ref, weight_obj_ref):
    count, side, _ = measured_ref.shape
    modes = probe_ref.shape[1] // side
    lanes = ext_ref.shape[2]
    grad_obj_ref[...] = jnp.zeros_like(grad_obj_ref)
    grad_probe_ref[...] = jnp.zeros_like(grad_probe_ref)
    weight_probe_ref[...] = jnp.zeros_like(weight_probe_ref)
    weight = jnp.zeros((side, side), jnp.float32)
    for m in range(modes):
        p_real = probe_ref[0, m * side : (m + 1) * side, :]
        p_imag = probe_ref[1, m * side : (m + 1) * side, :]
        weight += p_real * p_real + p_imag * p_imag
    weight_obj_ref[...] = weight

    def dot(left, right):
        return jnp.dot(left, right, preferred_element_type=jnp.float32)

    def two_sided(left_op, right_op, pair):
        half = dot(left_op[...], pair).astype(jnp.bfloat16)
        results = []
        for k in range(2):
            block = half[:, k * side : (k + 1) * side]
            rows = jnp.concatenate([block[:side], block[side:]], axis=1)
            results.append(dot(rows, right_op[...]))
        return results

    def visit(j, carry):
        row_at = places[j, 0]
        col_at = places[j, 1]
        tall = side + SUBLANES
        shift = lax.rem(row_at, SUBLANES)
        window = pl.ds(pl.multiple_of(row_at - shift, SUBLANES), tall)
        right = lax.rem(lanes - col_at, lanes)
        up = lax.rem(tall - shift, tall)

        def patch_of(i):
            columns = pltpu.roll(ext_ref[i, window, :], right, 1)[:, :side]
            return pltpu.roll(columns, up, 0)[:side]

        o_real = patch_of(0)
        o_imag = patch_of(1)
        weight_probe_ref[...] += o_real * o_real + o_imag * o_imag
        intensity = jnp.zeros((side, side), jnp.float32)
        for m in range(0, modes, 2):
            columns = []
            for k in (m, m + 1):
                p_real = probe_ref[0, k * side : (k + 1) * side, :]
                p_imag = probe_ref[1, k * side : (k + 1) * side, :]
                w_real = (p_real * o_real - p_imag * o_imag).astype(jnp.bfloat16)
                w_imag = (p_real * o_imag + p_imag * o_real).astype(jnp.bfloat16)
                columns.append(jnp.concatenate([w_real, w_imag], axis=0))
            for k, far in enumerate(two_sided(fwd_left, fwd_right, jnp.concatenate(columns, axis=1))):
                far_ref[(m + k) * side : (m + k + 1) * side, :] = far
                intensity += far[:, :side] * far[:, :side] + far[:, side:] * far[:, side:]
        shrink = 1.0 - measured_ref[j] / jnp.sqrt(intensity + SOFT_FLOOR)
        g_real = jnp.zeros((side, side), jnp.float32)
        g_imag = jnp.zeros((side, side), jnp.float32)
        for m in range(0, modes, 2):
            columns = []
            for k in (m, m + 1):
                rows = slice(k * side, (k + 1) * side)
                r_real = (far_ref[rows, :side] * shrink).astype(jnp.bfloat16)
                r_imag = (far_ref[rows, side:] * shrink).astype(jnp.bfloat16)
                columns.append(jnp.concatenate([r_real, r_imag], axis=0))
            for k, change in enumerate(two_sided(inv_left, inv_right, jnp.concatenate(columns, axis=1))):
                rows = slice((m + k) * side, (m + k + 1) * side)
                p_real = probe_ref[0, rows, :]
                p_imag = probe_ref[1, rows, :]
                c_real = change[:, :side]
                c_imag = change[:, side:]
                g_real += p_real * c_real + p_imag * c_imag
                g_imag += p_real * c_imag - p_imag * c_real
                grad_probe_ref[0, rows, :] += o_real * c_real + o_imag * c_imag
                grad_probe_ref[1, rows, :] += o_real * c_imag - o_imag * c_real
        short = jnp.zeros((SUBLANES, side), jnp.float32)
        blank = jnp.zeros((tall, lanes - side), jnp.float32)
        for i, part in enumerate((g_real, g_imag, weight_obj_ref[...])):
            part = jnp.concatenate([part, short], axis=0)
            wide = jnp.concatenate([pltpu.roll(part, shift, 0), blank], axis=1)
            grad_obj_ref[i, window, :] += pltpu.roll(wide, col_at, 1)
        return carry

    lax.fori_loop(0, count, visit, 0)


def flat(operators):
    left_op, right_op = operators
    side = left_op.shape[1]
    return (left_op.reshape(2 * side, 2 * side), right_op.reshape(2 * side, 2 * side))


def gradients(extended, probe, places, measured, forward, inverse):
    side = measured.shape[-1]
    vmem = pl.BlockSpec(memory_space=pltpu.VMEM)
    rows, lanes = extended.shape[1:]
    flops = measured.shape[0] * 4 * 2 * (2 * side) ** 2 * probe.shape[1]
    return pl.pallas_call(
        visit_kernel,
        out_shape=(
            jax.ShapeDtypeStruct((3, rows, lanes), jnp.float32),
            jax.ShapeDtypeStruct(probe.shape, jnp.float32),
            jax.ShapeDtypeStruct((side, side), jnp.float32),
        ),
        in_specs=[pl.BlockSpec(memory_space=pltpu.SMEM)] + [vmem] * 7,
        out_specs=(vmem, vmem, vmem),
        scratch_shapes=[
            pltpu.VMEM((probe.shape[1], 2 * side), jnp.float32),
            pltpu.VMEM((side, side), jnp.float32),
        ],
        compiler_params=pltpu.CompilerParams(vmem_limit_bytes=32 * 1024 * 1024),
        cost_estimate=pl.CostEstimate(flops=flops, bytes_accessed=4 * 1024 * 1024, transcendentals=0),
        name="visits",
    )(places, extended, probe, measured, *forward, *inverse)


def fold_rows(gradient, margin, tile_side):
    extent = gradient.shape[1]
    for direction in (1, -1):
        rim_part = gradient[:, extent - margin :, :] if direction == 1 else gradient[:, :margin, :]
        offset = margin if direction == 1 else tile_side
        arrived = from_behind(rim_part, "gy", direction)
        gradient = gradient.at[:, offset : offset + margin, :].add(arrived)
    return gradient[:, margin : margin + tile_side, :]


def fold_cols(gradient, margin, tile_side):
    extent = gradient.shape[2]
    for direction in (1, -1):
        rim_part = gradient[:, :, extent - margin :] if direction == 1 else gradient[:, :, :margin]
        offset = margin if direction == 1 else tile_side
        arrived = from_behind(rim_part, "gx", direction)
        gradient = gradient.at[:, :, offset : offset + margin].add(arrived)
    return gradient[:, :, margin : margin + tile_side]


def whole_of(own):
    planes, rows, side = own.shape
    blocks = own
    for axis in ("gy", "gx"):
        copies = jnp.broadcast_to(blocks[None], (lax.axis_size(axis), *blocks.shape))
        blocks = lax.all_to_all(copies, axis, 0, 0, tiled=True)
    return blocks.transpose(2, 1, 0, 3, 4).reshape(planes, -1, side)


def scattered_sum(terms):
    planes, rows, side = terms.shape
    down, across = lax.axis_size("gy"), lax.axis_size("gx")
    terms = terms.reshape(planes, down, across, rows // (down * across), side)
    terms = terms.transpose(2, 0, 1, 3, 4)
    terms = lax.all_to_all(terms, "gx", 0, 0, tiled=True).sum(axis=0)
    terms = terms.transpose(1, 0, 2, 3)
    return lax.all_to_all(terms, "gy", 0, 0, tiled=True).sum(axis=0)


def local(object_field, probe_modes, positions, amplitudes):
    probe_side = amplitudes.shape[-1]
    margin = probe_side // 2
    tile_side = object_field.shape[1]
    lanes = -(-(tile_side + probe_side) // 128) * 128
    places = positions.reshape(-1, 2)
    measured = amplitudes.reshape(-1, probe_side, probe_side)
    forward = flat(tables(probe_side, -1.0))
    inverse = flat(tables(probe_side, 1.0))
    own = probe_modes
    probe = whole_of(own)
    current = object_field
    for iteration in range(ITERS):
        extended = extended_2(current, (("gy", 1), ("gx", 2)), margin)
        extended = jnp.pad(extended, ((0, 0), (0, 0), (0, lanes - extended.shape[2])))
        grad_obj, grad_probe, weight_probe = gradients(
            extended, probe, places, measured, forward, inverse
        )
        grad_obj = grad_obj[:, :, : tile_side + probe_side]
        folded = fold_cols(fold_rows(grad_obj, margin, tile_side), margin, tile_side)
        current = current - folded[0:2] / (folded[2] + OBJECT_REG)
        weights = jnp.tile(weight_probe, (MODES, 1))[None]
        totals = scattered_sum(jnp.concatenate([grad_probe, weights]))
        own = own - totals[0:2] / (totals[2:3] + PROBE_REG)
        if iteration < ITERS - 1:
            probe = whole_of(own)
    return (current, own)


def solution(mesh):
    return jax.shard_map(
        local,
        mesh=mesh,
        in_specs=(
            P(None, "gy", "gx"),
            P(None, ("gy", "gx"), None),
            P("gy", "gx", None, None),
            P("gy", "gx", None, None, None),
        ),
        out_specs=(P(None, "gy", "gx"), P(None, ("gy", "gx"), None)),
        check_vma=False,
    )
```
